128 devices in a mesh: tier: 16 (over y, z), mat: 8 (over x, core).
Axes of the slice: x: 4, y: 4, z: 4, core: 2. Of those that a mesh axis runs over, the one named last changes fastest.
Arguments:
- costate: bfloat16 [512, 2, 256, 256], P(('tier', 'mat')), may hold values from -6 to 6
- hamiltonian: bfloat16 [256, 256], replicated, may hold values from -0.375 to 0.375
- couplers: bfloat16 [3, 256, 256], replicated, may hold values from -0.375 to 0.375
- damping: float32 [12], replicated, may hold values from 0.05 to 0.5
- coupling: float32 [2, 12], replicated, may hold values from -0.9 to 0.9
- levels: int32 [512, 12], P(('tier', 'mat')), may hold values from 0 to 3
- neighbour_slot: int32 [512, 24], P(('tier', 'mat')), may hold values from 0 to 31
- neighbour_mode: int32 [512, 24], P(('tier', 'mat')), may hold values from 0 to 11
- neighbour_flag: int32 [512, 24], P(('tier', 'mat')), may hold values from -1 to 1
- send_index: int32 [128, 32], P(('tier', 'mat')), may hold values from 0 to 3
Outputs:
- increment: float32 [512, 2, 256, 256], P(('tier', 'mat'))
- bath_gradient: float32 [12], replicated
The draws below stay inside these ranges and needn't reach their ends.
All inputs are finite; a program needn't handle non-finite values.
Results may differ from the reference program's by a relative error of at most 0.0053.
Values may be sent and summed in bfloat16 or wider, within the bound.
No kernel may reach another device: no remote copies, remote signals or barrier semaphores. Data moves between devices by JAX's collectives and lax.ppermute only.
A program may use at most 128 MiB of HBM per device.

```python
import math
import jax
import jax.numpy as jnp
from jax import lax

NL = 256
MODES = 12
OPS = 3
NEIGH = 24
CAP = 2
MB_DEV = 4
BLOCKS = 128
ADOS = 512
SLOTS = 32
N_MAT = 8


def set_ends(array, key, low, high):
    extent = array.shape
    spot = [jax.random.randint(jax.random.fold_in(key, axis), (), 0, extent[axis]) for axis in range(len(extent))]
    array = array.at[tuple(spot)].set(low)
    longest = extent.index(max(extent))
    spot[longest] = (spot[longest] + 1) % extent[longest]
    return array.at[tuple(spot)].set(high)


def steps_of(stream_key, extent, shards, low, largest):
    level = 1.0
    for dim, blocks in shards:
        heights = jax.random.uniform(jax.random.fold_in(jax.random.fold_in(stream_key, 6), dim), (blocks,), jnp.float32, low / len(shards), largest / len(shards))
        level = level * jnp.repeat(jnp.exp(heights), extent[dim] // blocks).reshape((-1,) + (1,) * (len(extent) - 1 - dim))
    return level


def noise(own_key, dims, spread, limit, cuts=(), kind=jnp.bfloat16):
    factor_of = steps_of(own_key, dims, cuts, -0.22, 0.18) if cuts else 1.0
    entries = jax.random.normal(own_key, dims, jnp.float32) * spread * factor_of
    return jnp.minimum(jnp.maximum(entries, -limit), limit).astype(kind)


def setup_inputs(seed: int = 0) -> dict:
    seeds = jax.random.split(jax.random.key(seed), 11)
    return {
        "costate": noise(seeds[0], (ADOS, 2, NL, NL), 1.0, 6.0, ((0, 128),)),
        "hamiltonian": noise(seeds[1], (NL, NL), NL ** -0.5, 0.375),
        "couplers": noise(seeds[2], (OPS, NL, NL), NL ** -0.5, 0.375),
        "damping": jnp.clip(jnp.exp(jax.random.uniform(seeds[3], (MODES,), jnp.float32, math.log(0.05), math.log(0.5))), 0.05, 0.5),
        "coupling": noise(seeds[4], (2, MODES), 0.3, 0.9, (), jnp.float32),
        "levels": set_ends(jax.random.randint(seeds[5], (ADOS, MODES), 0, 4), jax.random.fold_in(seeds[5], 1), 0, 3).astype(jnp.int32),
        "neighbour_slot": set_ends(jax.random.randint(seeds[6], (ADOS, NEIGH), 0, SLOTS), jax.random.fold_in(seeds[6], 1), 0, SLOTS - 1).astype(jnp.int32),
        "neighbour_mode": set_ends(jax.random.randint(seeds[7], (ADOS, NEIGH), 0, MODES), jax.random.fold_in(seeds[7], 1), 0, MODES - 1).astype(jnp.int32),
        "neighbour_flag": set_ends(jax.random.randint(seeds[8], (ADOS, NEIGH), -1, 2), jax.random.fold_in(seeds[8], 1), -1, 1).astype(jnp.int32),
        "send_index": set_ends(jax.random.randint(seeds[9], (BLOCKS, SLOTS), 0, MB_DEV), jax.random.fold_in(seeds[9], 1), 0, MB_DEV - 1).astype(jnp.int32),
    }


def symmetric(weight):
    square = weight.astype(jnp.float32)
    return ((square + jnp.swapaxes(square, -1, -2)) * 0.5).astype(jnp.bfloat16)

def evaluate(state, operators, damping, coupling, levels, neighbour_slot, neighbour_mode, neighbour_flag, send_index):
    high = lax.Precision.HIGHEST
    opfloat = operators.astype(jnp.float32)

    def single(index):
        block = index // MB_DEV
        tier_here = block // N_MAT
        group = block % N_MAT
        slot = neighbour_slot[index]
        provider = slot // CAP * N_MAT + group
        position = slot % CAP
        source = (provider * MB_DEV + send_index[provider, tier_here * CAP + position]).astype(jnp.int32)
        gathered = state[source].astype(jnp.float32)
        own = state[index].astype(jnp.float32)
        mode = neighbour_mode[index]
        flag = neighbour_flag[index]
        live = (flag >= 0).astype(jnp.float32)
        weight = jnp.sqrt(1.0 + levels[index][mode].astype(jnp.float32)) * live
        coup_real = coupling[0][mode] * weight
        coup_imag = coupling[1][mode] * weight
        right_imag = jnp.where(flag == 1, coup_imag, -coup_imag)
        select = (mode[None, :] % 3 == jnp.arange(3)[:, None]).astype(jnp.float32)

        def combine(real_part, imag_part):
            creal = select * real_part[None, :]
            cimag = select * imag_part[None, :]
            sreal = jnp.einsum('qe,eij->qij', creal, gathered[:, 0], precision=high) - jnp.einsum('qe,eij->qij', cimag, gathered[:, 1], precision=high)
            simag = jnp.einsum('qe,eij->qij', creal, gathered[:, 1], precision=high) + jnp.einsum('qe,eij->qij', cimag, gathered[:, 0], precision=high)
            return jnp.stack([sreal, simag], 1).astype(jnp.bfloat16)
        left_in = combine(coup_real, coup_imag)
        right_in = combine(coup_real, right_imag)
        rotated = jnp.stack([-state[index][1], state[index][0]])[None]
        left_all = jnp.concatenate([rotated, left_in], 0).astype(jnp.float32)
        right_all = jnp.concatenate([rotated, right_in], 0).astype(jnp.float32)
        left = jnp.einsum('oij,opjk->pik', opfloat, left_all, precision=high)
        right = jnp.einsum('opij,ojk->pik', right_all, opfloat, precision=high)
        decay = jnp.sum(levels[index].astype(jnp.float32) * damping)
        rate = left - right - decay * own
        correlation = jnp.einsum('pij,epij->e', own, gathered, precision=high)
        onehot = (mode[:, None] == jnp.arange(MODES)[None, :]).astype(jnp.float32)
        grad = jnp.dot(correlation * weight / NL, onehot, precision=high)
        return (rate, grad)
    rates, grads = lax.map(single, jnp.arange(state.shape[0], dtype=jnp.int32))
    return (rates, lax.optimization_barrier(jnp.sum(grads, 0)))

def reference(costate, hamiltonian, couplers, damping, coupling, levels, neighbour_slot, neighbour_mode, neighbour_flag, send_index):
    operators = jnp.concatenate([symmetric(hamiltonian)[None], symmetric(couplers)], 0)
    first, grad_first = evaluate(costate, operators, damping, coupling, levels, neighbour_slot, neighbour_mode, neighbour_flag, send_index)
    middle = (costate.astype(jnp.float32) + 0.125 * first).astype(jnp.bfloat16)
    second, grad_second = evaluate(middle, operators, damping, coupling, levels, neighbour_slot, neighbour_mode, neighbour_flag, send_index)
    return (0.25 * second, grad_first + grad_second)
```

```python
import jax
import jax.numpy as jnp
from jax import lax
from jax.experimental import pallas as pl
from jax.experimental.pallas import tpu as pltpu
from jax.sharding import Mesh
from jax.sharding import PartitionSpec as P

MODES = 12
OPS = 3
NEIGH = 24
NODES = 4
WIDTH = 256
HALF = 128
ROWS = 16
TIER_MAT = ("tier_0", "tier_1", "mat_0", "mat_1")
SMEM = pltpu.SMEM
ANY = pl.ANY
VMEM_LIMIT = 56 * 1024 * 1024


def smem():
    return pl.BlockSpec(memory_space=SMEM)


def anywhere():
    return pl.BlockSpec(memory_space=ANY)


def from_offset(value, axis, offset):
    return lax.ppermute(value, axis, [((i + offset) % 4, i) for i in range(4)])


def symmetric(weight):
    square = weight.astype(jnp.float32)
    return ((square + jnp.swapaxes(square, -1, -2)) * 0.5).astype(jnp.bfloat16)


def prepare_kernel(pos, slot, mode, flag, send_y, send_z, weights, counts, places, modes, values):
    y = pos[0]
    z = pos[1]
    here = (y * 4 + z) * 2

    def clear(i, carry):
        counts[i] = 0
        return carry

    lax.fori_loop(0, NODES * OPS * 2, clear, 0)

    def step(i, carry):
        n = i // NEIGH
        k = mode[i]
        f = flag[i]
        j = slot[i]

        @pl.when(f >= 0)
        def _():
            source = j // 2
            s = lax.rem(j, 2)
            dy = lax.rem(source // 4 - y + 4, 4)
            dz = lax.rem(lax.rem(source, 4) - z + 4, 4)
            at_a = jnp.where(
                dz == 0, dy * 4 + send_y[dy, here + s], 16 + (dz - 1) * 8 + dy * 2 + s
            )
            at_b = jnp.where(
                dy == 0, dz * 4 + send_z[dz, here + s], 16 + (dy - 1) * 8 + dz * 2 + s
            )
            which = (n * OPS + lax.rem(k, 3)) * 2 + f
            count = counts[which]
            at = which * NEIGH + count
            counts[which] = count + 1
            places[0, at] = at_a
            places[1, at] = at_b
            modes[at] = k
            values[0, at] = weights[0, n * MODES + k]
            values[1, at] = weights[1, n * MODES + k]
            values[2, at] = weights[2, n * MODES + k]

        return carry

    lax.fori_loop(0, NODES * NEIGH, step, 0)


def prepare(pos, slot, mode, flag, send_y, send_z, weights):
    lists = NODES * OPS * 2
    return pl.pallas_call(
        prepare_kernel,
        out_shape=(
            jax.ShapeDtypeStruct((lists,), jnp.int32),
            jax.ShapeDtypeStruct((2, lists * NEIGH), jnp.int32),
            jax.ShapeDtypeStruct((lists * NEIGH,), jnp.int32),
            jax.ShapeDtypeStruct((3, lists * NEIGH), jnp.float32),
        ),
        in_specs=[smem()] * 7,
        out_specs=(smem(),) * 4,
        cost_estimate=pl.CostEstimate(flops=2000000, bytes_accessed=20000, transcendentals=0),
        name="prepare",
    )(pos, slot, mode, flag, send_y, send_z, weights)


def pick_kernel(hop, pos, send_y, send_z, *refs):
    a_in = refs[0:4]
    b_in = refs[4:8]
    a_out, b_out, room, in_sem, out_sem = refs[8:]
    y = pos[0]
    z = pos[1]
    there_a = (y * 4 + lax.rem(z + hop, 4)) * 2
    there_b = (lax.rem(y + hop, 4) * 4 + z) * 2
    reads = []
    writes = []
    for d in range(4):
        for s in range(2):
            at = d * 2 + s
            for half, (ins, out, send, there) in enumerate(
                ((a_in, a_out, send_y, there_a), (b_in, b_out, send_z, there_b))
            ):
                slot = half * 8 + at
                reads.append(
                    pltpu.make_async_copy(ins[d].at[send[d, there + s]], room.at[slot], in_sem.at[slot])
                )
                writes.append(pltpu.make_async_copy(room.at[slot], out.at[at], out_sem.at[slot]))
    for read in reads:
        read.start()
    for read, write in zip(reads, writes):
        read.wait()
        write.start()
    for write in writes:
        write.wait()


def pick(hop, pos, send_y, send_z, a_parts, b_parts):
    shape = jax.ShapeDtypeStruct((8, 2, HALF, WIDTH), jnp.bfloat16)
    return pl.pallas_call(
        lambda *refs: pick_kernel(hop, *refs),
        out_shape=(shape, shape),
        in_specs=[smem()] * 3 + [anywhere()] * 8,
        out_specs=(anywhere(), anywhere()),
        scratch_shapes=[
            pltpu.VMEM((16, 2, HALF, WIDTH), jnp.bfloat16),
            pltpu.SemaphoreType.DMA((16,)),
            pltpu.SemaphoreType.DMA((16,)),
        ],
        compiler_params=pltpu.CompilerParams(vmem_limit_bytes=VMEM_LIMIT),
        cost_estimate=pl.CostEstimate(flops=3000000, bytes_accessed=4 << 20, transcendentals=0),
        name="pick",
    )(pos, send_y, send_z, *a_parts, *b_parts)


def rate_kernel(last, counts, places, modes, values, decay, own, operators, *refs):
    sources = refs[0:14]
    out, grads, buffer, left, right, totals, sems = refs[14:]
    n = pl.program_id(0)

    @pl.when(n == 0)
    def _():
        copies = []
        for half in range(2):
            at = 0
            for part in range(7):
                ref = sources[half * 7 + part]
                size = ref.shape[0]
                copies.append(
                    pltpu.make_async_copy(
                        ref, buffer.at[half, pl.ds(at, size)], sems.at[half * 7 + part]
                    )
                )
                at += size
        for copy in copies:
            copy.start()
        totals[...] = jnp.zeros_like(totals)
        for copy in copies:
            copy.wait()

    for half in range(2):

        def block(i, carry, half=half):
            row = pl.multiple_of(i * ROWS, ROWS)
            full = pl.multiple_of(half * HALF + i * ROWS, ROWS)
            own_real = own[0, 0, pl.ds(full, ROWS), :].astype(jnp.float32)
            own_imag = own[0, 1, pl.ds(full, ROWS), :].astype(jnp.float32)
            zero = jnp.zeros((ROWS, WIDTH), jnp.float32)
            left[0, pl.ds(full, ROWS), :] = (-own_imag).astype(jnp.bfloat16)
            left[1, pl.ds(full, ROWS), :] = own_real.astype(jnp.bfloat16)
            right[0, pl.ds(full, ROWS), 0:WIDTH] = (-own_imag).astype(jnp.bfloat16)
            right[1, pl.ds(full, ROWS), 0:WIDTH] = own_real.astype(jnp.bfloat16)
            for q in range(OPS):

                def load(at):
                    place = places[half, at]
                    real = buffer[half, place, 0, pl.ds(row, ROWS), :].astype(jnp.float32)
                    imag = buffer[half, place, 1, pl.ds(row, ROWS), :].astype(jnp.float32)
                    product = own_real * real + own_imag * imag
                    product = product[0:8] + product[8:16]
                    product = product[:, 0:128] + product[:, 128:256]
                    mode = modes[at]
                    totals[mode] = totals[mode] + values[0, at] * product
                    return real, imag, values[1, at], values[2, at]

                which = (n * OPS + q) * 2

                def raised(e, sums):
                    sum_real, sum_imag = sums
                    real, imag, u, v = load((which + 1) * NEIGH + e)
                    return sum_real + (u * real - v * imag), sum_imag + (u * imag + v * real)

                def lowered(e, sums):
                    sum_real, sum_imag, turn_real, turn_imag = sums
                    real, imag, u, v = load(which * NEIGH + e)
                    return (
                        sum_real + u * real,
                        sum_imag + u * imag,
                        turn_real + v * real,
                        turn_imag + v * imag,
                    )

                sum_real, sum_imag = lax.fori_loop(0, counts[which + 1], raised, (zero, zero))
                sum_real, sum_imag, turn_real, turn_imag = lax.fori_loop(
                    0, counts[which], lowered, (sum_real, sum_imag, zero, zero)
                )
                at_row = pl.multiple_of((q + 1) * WIDTH + full, ROWS)
                column = (q + 1) * WIDTH
                left[0, pl.ds(at_row, ROWS), :] = (sum_real - turn_imag).astype(jnp.bfloat16)
                left[1, pl.ds(at_row, ROWS), :] = (sum_imag + turn_real).astype(jnp.bfloat16)
                right[0, pl.ds(full, ROWS), column : column + WIDTH] = (
                    sum_real + turn_imag
                ).astype(jnp.bfloat16)
                right[1, pl.ds(full, ROWS), column : column + WIDTH] = (
                    sum_imag - turn_real
                ).astype(jnp.bfloat16)
            return carry

        lax.fori_loop(0, HALF // ROWS, block, 0)

    rate_decay = decay[n]
    for part in range(2):
        total = jnp.zeros((WIDTH, WIDTH), jnp.float32)
        minus = jnp.zeros((WIDTH, WIDTH), jnp.float32)
        for q in range(OPS + 1):
            cut = slice(q * WIDTH, (q + 1) * WIDTH)
            total += jnp.dot(operators[q], left[part, cut, :], preferred_element_type=jnp.float32)
            minus += jnp.dot(right[part, :, cut], operators[q], preferred_element_type=jnp.float32)
        state = own[0, part].astype(jnp.float32)
        rate = total - minus - rate_decay * state
        if last:
            out[0, part] = 0.25 * rate
        else:
            out[0, part] = (state + 0.125 * rate).astype(jnp.bfloat16)

    @pl.when(n == NODES - 1)
    def _():
        summed = jnp.sum(totals[...], axis=1)
        summed = jnp.sum(summed, axis=1, keepdims=True) * (1.0 / WIDTH)
        grads[...] = jnp.broadcast_to(summed, (MODES, 128))


def rates(last, lists, decay, state, operators, sources):
    kind = jnp.float32 if last else jnp.bfloat16
    counts, places, modes, values = lists
    whole = (1, 2, WIDTH, WIDTH)
    return pl.pallas_call(
        lambda *refs: rate_kernel(last, *refs),
        grid=(NODES,),
        out_shape=(
            jax.ShapeDtypeStruct((NODES, 2, WIDTH, WIDTH), kind),
            jax.ShapeDtypeStruct((MODES, 128), jnp.float32),
        ),
        in_specs=[smem()] * 5
        + [
            pl.BlockSpec(whole, lambda n: (n, 0, 0, 0)),
            pl.BlockSpec((OPS + 1, WIDTH, WIDTH), lambda n: (0, 0, 0)),
        ]
        + [anywhere()] * 14,
        out_specs=(
            pl.BlockSpec(whole, lambda n: (n, 0, 0, 0)),
            pl.BlockSpec((MODES, 128), lambda n: (0, 0)),
        ),
        scratch_shapes=[
            pltpu.VMEM((2, 40, 2, HALF, WIDTH), jnp.bfloat16),
            pltpu.VMEM((2, (OPS + 1) * WIDTH, WIDTH), jnp.bfloat16),
            pltpu.VMEM((2, WIDTH, (OPS + 1) * WIDTH), jnp.bfloat16),
            pltpu.VMEM((MODES, 8, 128), jnp.float32),
            pltpu.SemaphoreType.DMA((14,)),
        ],
        compiler_params=pltpu.CompilerParams(
            vmem_limit_bytes=VMEM_LIMIT, dimension_semantics=("arbitrary",)
        ),
        cost_estimate=pl.CostEstimate(
            flops=2 * 2 * 4 * 4 * 2 * WIDTH**3, bytes_accessed=14 << 20, transcendentals=0
        ),
        name="rates",
    )(counts, places, modes, values, decay, state, operators, *sources)


def over_all(value):
    value = value + lax.ppermute(value, "mat_1", [(0, 1), (1, 0)])
    for axis in ("mat_0", "tier_1", "tier_0"):
        one = from_offset(value, axis, 1)
        three = from_offset(value, axis, 3)
        two = from_offset(value, axis, 2)
        value = (value + two) + (one + three)
    return value


def per_device(
    costate,
    hamiltonian,
    couplers,
    damping,
    coupling,
    levels,
    neighbour_slot,
    neighbour_mode,
    neighbour_flag,
    send_index,
):
    high = lax.Precision.HIGHEST
    y = lax.axis_index("tier_0")
    z = lax.axis_index("tier_1")
    pos = jnp.stack([y, z]).astype(jnp.int32)
    own_send = send_index[0]
    send_y = jnp.stack([own_send] + [from_offset(own_send, "tier_0", d) for d in (1, 2, 3)])
    send_z = jnp.stack([own_send] + [from_offset(own_send, "tier_1", d) for d in (1, 2, 3)])
    operators = jnp.concatenate([symmetric(hamiltonian)[None], symmetric(couplers)], 0)
    depth = levels.astype(jnp.float32)
    weight = jnp.sqrt(1.0 + depth)
    weights = jnp.stack([weight, weight * coupling[0], weight * coupling[1]]).reshape(3, -1)
    decay = jnp.sum(depth * damping, axis=1)
    lists = prepare(
        pos,
        neighbour_slot.reshape(-1),
        neighbour_mode.reshape(-1),
        neighbour_flag.reshape(-1),
        send_y,
        send_z,
        weights,
    )

    def section(state, last):
        half_a = state[:, :, :HALF, :]
        half_b = state[:, :, HALF:, :]
        a_parts = [half_a] + [from_offset(half_a, "tier_0", d) for d in (1, 2, 3)]
        b_parts = [half_b] + [from_offset(half_b, "tier_1", d) for d in (1, 2, 3)]
        a_far = {}
        b_far = {}
        for hop in (1, 3, 2):
            a_out, b_out = pick(hop, pos, send_y, send_z, a_parts, b_parts)
            a_far[4 - hop] = from_offset(a_out, "tier_1", 4 - hop)
            b_far[4 - hop] = from_offset(b_out, "tier_0", 4 - hop)
        sources = a_parts + [a_far[d] for d in (1, 2, 3)] + b_parts + [b_far[d] for d in (1, 2, 3)]
        return rates(last, lists, decay, state, operators, sources)

    middle, grad_first = section(costate, False)
    increment, grad_second = section(middle, True)
    gradient = over_all(grad_first + grad_second)
    return (increment, gradient[:, 0])


def solution(mesh):
    finer = Mesh(mesh.devices.reshape(4, 4, 4, 2), TIER_MAT)
    return jax.shard_map(
        per_device,
        mesh=finer,
        in_specs=(
            P(TIER_MAT, None, None, None),
            P(),
            P(),
            P(),
            P(),
            P(TIER_MAT, None),
            P(TIER_MAT, None),
            P(TIER_MAT, None),
            P(TIER_MAT, None),
            P(TIER_MAT, None),
        ),
        out_specs=(P(TIER_MAT, None, None, None), P()),
        check_vma=False,
    )
```

```python
import math

import jax
import jax.numpy as jnp
from jax import lax
from jax.experimental import pallas as pl
from jax.experimental.pallas import tpu as pltpu
from jax.sharding import Mesh
from jax.sharding import PartitionSpec as P


MODES = 12
OPS = 3
NEIGH = 24
NODES = 4
SLOTS = 32
WIDTH = 256
HALF = 128
CHUNKS = 2
PIECE = HALF // CHUNKS
ROWS = 32
HOPS = (2, 1, 3)
LISTS = NODES * OPS * 2
ROOM = (LISTS + 1) * NEIGH
PART = 2 * PIECE
BLOCK = 2 * PART
TIER_MAT = ("tier_0", "tier_1", "mat_0", "mat_1")
SMEM = pltpu.SMEM
ANY = pl.ANY
VMEM_LIMIT = 67043328


def smem():
    return pl.BlockSpec(memory_space=SMEM)


def anywhere():
    return pl.BlockSpec(memory_space=ANY)


def from_offset(value, axis, offset):
    return lax.ppermute(value, axis, [((i + offset) % 4, i) for i in range(4)])


def joint(value, step, cross):
    pairs = []
    for y in range(4):
        for z in range(4):
            for core in range(2):
                if core == cross:
                    to = ((y + step) % 4 * 4 + z) * 2 + core
                else:
                    to = (y * 4 + (z + step) % 4) * 2 + core
                pairs.append(((y * 4 + z) * 2 + core, to))
    return lax.ppermute(value, ("tier_0", "tier_1", "mat_1"), pairs)


def root_of(level):
    high = jnp.where(level == 3, 2.0, math.sqrt(3.0))
    low = jnp.where(level == 1, math.sqrt(2.0), 1.0)
    return jnp.where(level >= 2, high, low).astype(jnp.float32)


def place_of(along, across, s, near):
    return jnp.where(across == 0, along * 4 + near, 16 + (across - 1) * 8 + along * 2 + s)


def position():
    return lax.axis_index("tier_0"), lax.axis_index("tier_1"), lax.axis_index("mat_1")


def prepare_kernel(
    slot,
    mode,
    flag,
    send,
    levels,
    damping,
    coupling,
    hamiltonian,
    couplers,
    counts,
    codes,
    values,
    decay,
    operators,
    table,
):
    for q in range(OPS + 1):
        raw = (hamiltonian[...] if q == 0 else couplers[q - 1]).astype(jnp.float32)
        operators[q * WIDTH : (q + 1) * WIDTH] = ((raw + raw.T) * 0.5).astype(jnp.bfloat16)

    y, z, core = position()
    here = (y * 4 + z) * 2
    for i in range(LISTS + 1):
        counts[i] = 0
    for n in range(NODES):
        rate = levels[n, 0].astype(jnp.float32) * damping[0]
        for k in range(1, MODES):
            rate += levels[n, k].astype(jnp.float32) * damping[k]
        decay[n] = rate

    def tabulate(source, carry):
        dy = lax.rem(source // 4 - y + 4, 4)
        dz = lax.rem(lax.rem(source, 4) - z + 4, 4)
        along = jnp.where(core == 0, dy, dz)
        across = jnp.where(core == 0, dz, dy)
        for s in range(2):
            near = send[along * SLOTS + here + s]
            table[source * 2 + s] = place_of(along, across, s, near)
        return carry

    lax.fori_loop(0, SLOTS // 2, tabulate, 0)

    def step(e, carry):
        for n in range(NODES):
            k = mode[n, e]
            f = flag[n, e]
            j = slot[n, e]
            w = root_of(levels[n, k])
            which = jnp.where(f >= 0, (n * OPS + lax.rem(k, 3)) * 2 + f, LISTS)
            count = counts[which]
            at = which * NEIGH + jnp.where(f >= 0, count, 0)
            counts[which] = count + 1
            codes[at] = table[j]
            codes[ROOM + at] = k
            values[at] = w
            values[ROOM + at] = w * coupling[0, k]
            values[2 * ROOM + at] = w * coupling[1, k]
        return carry

    lax.fori_loop(0, NEIGH, step, 0)


def prepare(slot, mode, flag, send, levels, damping, coupling, hamiltonian, couplers):
    return pl.pallas_call(
        prepare_kernel,
        out_shape=(
            jax.ShapeDtypeStruct((LISTS + 1,), jnp.int32),
            jax.ShapeDtypeStruct((2 * ROOM,), jnp.int32),
            jax.ShapeDtypeStruct((3 * ROOM,), jnp.float32),
            jax.ShapeDtypeStruct((NODES,), jnp.float32),
            jax.ShapeDtypeStruct(((OPS + 1) * WIDTH, WIDTH), jnp.bfloat16),
        ),
        in_specs=[smem()] * 7 + [pl.BlockSpec(memory_space=pltpu.VMEM)] * 2,
        out_specs=(smem(),) * 4 + (pl.BlockSpec(memory_space=pltpu.VMEM),),
        scratch_shapes=[SMEM((SLOTS,), jnp.int32)],
        cost_estimate=pl.CostEstimate(flops=2000000, bytes_accessed=20000, transcendentals=0),
        name="prepare",
    )(slot, mode, flag, send, levels, damping, coupling, hamiltonian, couplers)


def copy_through(reads, writes):
    for read in reads:
        read.start()
    for read, write in zip(reads, writes):
        read.wait()
        write.start()
    for write in writes:
        write.wait()


def across(hop):
    y, z, core = position()
    along_z = y * 4 + lax.rem(z + hop, 4)
    along_y = lax.rem(y + hop, 4) * 4 + z
    return jnp.where(core == 0, along_z, along_y) * 2


def pick_kernel(send, *refs):
    ins = refs[0:4]
    outs = refs[4:7]
    room, in_sem, out_sem = refs[7:]
    reads = []
    writes = []
    for i, hop in enumerate(HOPS):
        there = across(hop)
        for d in range(4):
            for s in range(2):
                at = d * 2 + s
                slot = i * 8 + at
                row = pl.multiple_of(send[d * SLOTS + there + s] * BLOCK, BLOCK)
                reads.append(
                    pltpu.make_async_copy(
                        ins[d].at[pl.ds(row, BLOCK)], room.at[slot], in_sem.at[slot]
                    )
                )
                writes.append(
                    pltpu.make_async_copy(room.at[slot], outs[i].at[at], out_sem.at[slot])
                )
    copy_through(reads, writes)


def pick(send, parts):
    shape = jax.ShapeDtypeStruct((8, BLOCK, WIDTH), jnp.bfloat16)
    return pl.pallas_call(
        pick_kernel,
        out_shape=(shape,) * 3,
        in_specs=[smem()] + [anywhere()] * 4,
        out_specs=(anywhere(),) * 3,
        scratch_shapes=[
            pltpu.VMEM((24, BLOCK, WIDTH), jnp.bfloat16),
            pltpu.SemaphoreType.DMA((24,)),
            pltpu.SemaphoreType.DMA((24,)),
        ],
        compiler_params=pltpu.CompilerParams(vmem_limit_bytes=VMEM_LIMIT),
        cost_estimate=pl.CostEstimate(flops=3000000, bytes_accessed=6 << 20, transcendentals=0),
        name="pick",
    )(send, *parts)


def row_of(chunk, half):
    return chunk * 2 * PIECE + half * PIECE


def rate_kernel(chunk, last, counts, codes, values, decay, operators_from, *refs):
    final = chunk == CHUNKS - 1
    own_from = refs[0:CHUNKS]
    refs = refs[CHUNKS:]
    if chunk > 0:
        before_from = refs[0]
        refs = refs[1:]
    sources = refs[0:7]
    refs = refs[7:]
    outs = CHUNKS if final and not last else 1
    out = refs[0:outs]
    grads, buffer, left, right, held, totals, sems, own, operators, *rest = refs[outs:]
    n = pl.program_id(0)

    copies = ([], [])
    for half in range(2):
        moves = []
        rows = pl.ds(half * PART, PART)
        for part in range(7):
            ref = sources[part]
            if part < 4:
                for m in range(NODES):
                    from_rows = pl.ds(m * BLOCK + half * PART, PART)
                    moves.append((ref.at[from_rows], buffer.at[part * 4 + m, rows]))
            else:
                places = pl.ds(16 + (part - 4) * 8, 8)
                moves.append((ref.at[:, rows], buffer.at[places, rows]))
        for i, (ref, to) in enumerate(moves):
            copies[half].append(pltpu.make_async_copy(ref, to, sems.at[half * 19 + i]))

    own_copies = [
        pltpu.make_async_copy(
            own_from[c].at[pl.ds(0, NODES * BLOCK)], own.at[c], sems.at[38 + c]
        )
        for c in range(CHUNKS)
    ]
    late_copies = [pltpu.make_async_copy(operators_from, operators, sems.at[38 + CHUNKS])]
    if chunk > 0:
        before = rest[0]
        late_copies.append(pltpu.make_async_copy(before_from, before, sems.at[39 + CHUNKS]))

    @pl.when(n == 0)
    def _():
        for copy in own_copies + copies[0] + copies[1] + late_copies:
            copy.start()
        totals[...] = jnp.zeros_like(totals)

    for half in range(2):
        mine = own.at[chunk, pl.ds(pl.multiple_of(n * BLOCK, BLOCK), BLOCK)]
        base = half * PART

        @pl.when(n == 0)
        def _(half=half):
            for copy in own_copies * (half == 0) + copies[half]:
                copy.wait()

        def block(i, carry, half=half, mine=mine, base=base):
            row = pl.multiple_of(i * ROWS, ROWS)
            here = pl.multiple_of(half * PIECE + i * ROWS, ROWS)
            own_real = mine[pl.ds(base + row, ROWS), :].astype(jnp.float32)
            own_imag = mine[pl.ds(base + PIECE + row, ROWS), :].astype(jnp.float32)
            held[0] = own_real
            held[1] = own_imag
            zero = jnp.zeros((ROWS, WIDTH), jnp.float32)
            left[0, pl.ds(here, ROWS), :] = (-own_imag).astype(jnp.bfloat16)
            left[1, pl.ds(here, ROWS), :] = own_real.astype(jnp.bfloat16)
            right[0, pl.ds(here, ROWS), 0:WIDTH] = (-own_imag).astype(jnp.bfloat16)
            right[1, pl.ds(here, ROWS), 0:WIDTH] = own_real.astype(jnp.bfloat16)
            for q in range(OPS):

                def entry(at):
                    place = codes[at]
                    mode = codes[ROOM + at]
                    return place, mode, values[at], values[ROOM + at], values[2 * ROOM + at]

                def load(now):
                    place, mode, w, u, v = now
                    real = buffer[place, pl.ds(half * PART + row, ROWS), :].astype(jnp.float32)
                    imag = buffer[place, pl.ds(half * PART + PIECE + row, ROWS), :].astype(jnp.float32)
                    product = held[0] * real + held[1] * imag
                    product = product[:, 0:128] + product[:, 128:256]
                    product = jnp.sum(product.reshape(ROWS // 8, 8, 128), axis=0)
                    totals[mode] = totals[mode] + w * product
                    return real, imag, u, v

                which = (n * OPS + q) * 2

                def raised(e, carry):
                    now, sum_real, sum_imag = carry
                    after = entry((which + 1) * NEIGH + e + 1)
                    real, imag, u, v = load(now)
                    return (
                        after,
                        sum_real + (u * real - v * imag),
                        sum_imag + (u * imag + v * real),
                    )

                def lowered(e, carry):
                    now, sum_real, sum_imag, turn_real, turn_imag = carry
                    after = entry(which * NEIGH + e + 1)
                    real, imag, u, v = load(now)
                    return (
                        after,
                        sum_real + u * real,
                        sum_imag + u * imag,
                        turn_real + v * real,
                        turn_imag + v * imag,
                    )

                start = entry((which + 1) * NEIGH)
                start_lowered = entry(which * NEIGH)
                _, sum_real, sum_imag = lax.fori_loop(
                    0, counts[which + 1], raised, (start, zero, zero)
                )
                _, sum_real, sum_imag, turn_real, turn_imag = lax.fori_loop(
                    0, counts[which], lowered, (start_lowered, sum_real, sum_imag, zero, zero)
                )
                at_row = pl.multiple_of((q + 1) * 2 * PIECE + here, ROWS)
                column = (q + 1) * WIDTH
                left[0, pl.ds(at_row, ROWS), :] = (sum_real - turn_imag).astype(jnp.bfloat16)
                left[1, pl.ds(at_row, ROWS), :] = (sum_imag + turn_real).astype(jnp.bfloat16)
                right[0, pl.ds(here, ROWS), column : column + WIDTH] = (
                    sum_real + turn_imag
                ).astype(jnp.bfloat16)
                right[1, pl.ds(here, ROWS), column : column + WIDTH] = (
                    sum_imag - turn_real
                ).astype(jnp.bfloat16)
            return carry

        lax.fori_loop(0, PIECE // ROWS, block, 0)

    @pl.when(n == 0)
    def _():
        for copy in late_copies:
            copy.wait()

    rate_decay = decay[n]
    columns = slice(chunk * 2 * PIECE, (chunk + 1) * 2 * PIECE)
    op_left = jnp.concatenate(
        [operators[q * WIDTH : (q + 1) * WIDTH, columns] for q in range(OPS + 1)], axis=1
    )
    for part in range(2):
        total = jnp.dot(op_left, left[part], preferred_element_type=jnp.float32)
        minus = jnp.dot(right[part], operators[...], preferred_element_type=jnp.float32)
        if chunk > 0:
            total += before[n, part]
        for c in range(CHUNKS):
            for half in range(2):
                rows = slice(row_of(c, half), row_of(c, half) + PIECE)
                value = total[rows]
                if c == chunk or (final and not last):
                    at = half * PART + part * PIECE
                    state = own[c, pl.ds(pl.multiple_of(n * BLOCK + at, PIECE), PIECE)].astype(
                        jnp.float32
                    )
                if c == chunk:
                    value -= minus[half * PIECE : (half + 1) * PIECE] + rate_decay * state
                if not final:
                    out[0][0, part, rows] = value
                elif last:
                    out[0][0, part, rows] = 0.25 * value
                else:
                    out[c][at : at + PIECE] = (state + 0.125 * value).astype(jnp.bfloat16)

    @pl.when(n == NODES - 1)
    def _():
        summed = jnp.sum(totals[...], axis=1)
        summed = jnp.sum(summed, axis=1, keepdims=True) * (1.0 / WIDTH)
        grads[...] = jnp.broadcast_to(summed, (MODES, 128))


def rates(chunk, last, lists, decay, operators, own, before, sources):
    final = chunk == CHUNKS - 1
    counts, codes, values = lists
    whole = pl.BlockSpec((1, 2, WIDTH, WIDTH), lambda n: (n, 0, 0, 0))
    block = pl.BlockSpec((BLOCK, WIDTH), lambda n: (n, 0))
    if final and not last:
        outs = (jax.ShapeDtypeStruct((NODES * BLOCK, WIDTH), jnp.bfloat16),) * CHUNKS
        out_specs = (block,) * CHUNKS
    else:
        outs = (jax.ShapeDtypeStruct((NODES, 2, WIDTH, WIDTH), jnp.float32),)
        out_specs = (whole,)
    return pl.pallas_call(
        lambda *refs: rate_kernel(chunk, last, *refs),
        grid=(NODES,),
        out_shape=outs + (jax.ShapeDtypeStruct((MODES, 128), jnp.float32),),
        in_specs=[smem()] * 4
        + [anywhere()] * (8 + CHUNKS + (chunk > 0)),
        out_specs=out_specs + (pl.BlockSpec((MODES, 128), lambda n: (0, 0)),),
        scratch_shapes=[
            pltpu.VMEM((40, 2 * PART, WIDTH), jnp.bfloat16),
            pltpu.VMEM((2, (OPS + 1) * 2 * PIECE, WIDTH), jnp.bfloat16),
            pltpu.VMEM((2, 2 * PIECE, (OPS + 1) * WIDTH), jnp.bfloat16),
            pltpu.VMEM((2, ROWS, WIDTH), jnp.float32),
            pltpu.VMEM((MODES, 8, 128), jnp.float32),
            pltpu.SemaphoreType.DMA((40 + CHUNKS,)),
            pltpu.VMEM((CHUNKS, NODES * BLOCK, WIDTH), jnp.bfloat16),
            pltpu.VMEM(operators.shape, jnp.bfloat16),
        ]
        + [pltpu.VMEM((NODES, 2, WIDTH, WIDTH), jnp.float32)] * (chunk > 0),
        compiler_params=pltpu.CompilerParams(
            vmem_limit_bytes=VMEM_LIMIT, dimension_semantics=("arbitrary",)
        ),
        cost_estimate=pl.CostEstimate(
            flops=2 * 2 * 4 * 4 * WIDTH**3, bytes_accessed=8 << 20, transcendentals=0
        ),
        name="rates",
    )(counts, codes, values, decay, operators, *own, *before, *sources)


def over_all(value):
    value = value + lax.ppermute(value, "mat_1", [(0, 1), (1, 0)])
    for axis in ("mat_0", "tier_1", "tier_0"):
        one = from_offset(value, axis, 1)
        three = from_offset(value, axis, 3)
        two = from_offset(value, axis, 2)
        value = (value + two) + (one + three)
    return value


def per_device(
    costate,
    hamiltonian,
    couplers,
    damping,
    coupling,
    levels,
    neighbour_slot,
    neighbour_mode,
    neighbour_flag,
    send_index,
):
    split = costate.reshape(NODES, 2, CHUNKS, 2, PIECE, WIDTH).transpose(2, 0, 3, 1, 4, 5)
    split = split.reshape(CHUNKS, NODES * BLOCK, WIDTH)
    label = jnp.pad(send_index.astype(jnp.bfloat16), ((0, 15), (0, WIDTH - SLOTS)))
    start = [jnp.concatenate([split[0], label])] + [split[c] for c in range(1, CHUNKS)]

    def section(own, last, tables):
        rings = []
        for c in range(CHUNKS):
            parts = [own[c]] * 4
            for offset in (2, 1, 3):
                parts[offset] = joint(own[c], 4 - offset, 0)
            rings.append(parts)
        if tables is None:
            held = lax.optimization_barrier(rings[0])
            send = jnp.concatenate([part[NODES * BLOCK, :SLOTS] for part in held]).astype(jnp.int32)
            *lists, decay, operators = prepare(
                neighbour_slot,
                neighbour_mode,
                neighbour_flag,
                send,
                levels,
                damping,
                coupling,
                hamiltonian,
                couplers,
            )
            tables = (send, lists, decay, operators)
        send, lists, decay, operators = tables
        far = []
        for c in range(CHUNKS):
            picked = pick(send, rings[c])
            come = {}
            for i, hop in enumerate(HOPS):
                come[4 - hop] = joint(picked[i], hop, 1)
            far.append(come)
        grads = 0.0
        before = ()
        for c in range(CHUNKS):
            sources = rings[c] + [far[c][d] for d in (1, 2, 3)]
            *before, grad = rates(c, last, lists, decay, operators, own, before, sources)
            grads = grads + grad
        return before, grads, tables

    middle, grad_first, tables = section(start, False, None)
    (increment,), grad_second, _ = section(middle, True, tables)
    gradient = over_all(grad_first + grad_second)
    return (increment, gradient[:, 0])


def solution(mesh):
    finer = Mesh(mesh.devices.reshape(4, 4, 4, 2), TIER_MAT)
    return jax.shard_map(
        per_device,
        mesh=finer,
        in_specs=(
            P(TIER_MAT, None, None, None),
            P(),
            P(),
            P(),
            P(),
            P(TIER_MAT, None),
            P(TIER_MAT, None),
            P(TIER_MAT, None),
            P(TIER_MAT, None),
            P(TIER_MAT, None),
        ),
        out_specs=(P(TIER_MAT, None, None, None), P()),
        check_vma=False,
    )
```

```python
import math

import jax
import jax.numpy as jnp
from jax import lax
from jax.experimental import pallas as pl
from jax.experimental.pallas import tpu as pltpu
from jax.sharding import Mesh
from jax.sharding import PartitionSpec as P


MODES = 12
OPS = 3
NEIGH = 24
NODES = 4
DEVICES = 128
SLOTS = 32
WIDTH = 256
HALF = 128
CHUNKS = 2
PIECE = HALF // CHUNKS
ROWS = 32
HOPS = (1, 3, 2)
LISTS = NODES * OPS * 2
ROOM = (LISTS + 1) * NEIGH
PART = 2 * PIECE
BLOCK = 2 * PART
TIER_MAT = ("tier_0", "tier_1", "mat_0", "mat_1")
SMEM = pltpu.SMEM
ANY = pl.ANY
VMEM_LIMIT = 67043328


def smem():
    return pl.BlockSpec(memory_space=SMEM)


def anywhere():
    return pl.BlockSpec(memory_space=ANY)


def joint(value, step, cross):
    pairs = []
    for y in range(4):
        for z in range(4):
            for core in range(2):
                if core == cross:
                    to = ((y + step) % 4 * 4 + z) * 2 + core
                else:
                    to = (y * 4 + (z + step) % 4) * 2 + core
                pairs.append(((y * 4 + z) * 2 + core, to))
    return lax.ppermute(value, ("tier_0", "tier_1", "mat_1"), pairs)


def root_of(level):
    high = jnp.where(level == 3, 2.0, math.sqrt(3.0))
    low = jnp.where(level == 1, math.sqrt(2.0), 1.0)
    return jnp.where(level >= 2, high, low).astype(jnp.float32)


def place_of(along, across, s, near):
    return jnp.where(across == 0, along * 4 + near, 16 + (across - 1) * 8 + along * 2 + s)


def position():
    return lax.axis_index("tier_0"), lax.axis_index("tier_1"), lax.axis_index("mat_1")


def prepare_kernel(
    slot,
    mode,
    flag,
    send,
    levels,
    damping,
    coupling,
    hamiltonian,
    couplers,
    counts,
    codes,
    values,
    decay,
    operators,
    table,
):
    for q in range(OPS + 1):
        raw = (hamiltonian[...] if q == 0 else couplers[q - 1]).astype(jnp.float32)
        operators[q * WIDTH : (q + 1) * WIDTH] = ((raw + raw.T) * 0.5).astype(jnp.bfloat16)

    y, z, core = position()
    here = (y * 4 + z) * 2
    for i in range(LISTS + 1):
        counts[i] = 0
    for n in range(NODES):
        rate = levels[n, 0].astype(jnp.float32) * damping[0]
        for k in range(1, MODES):
            rate += levels[n, k].astype(jnp.float32) * damping[k]
        decay[n] = rate

    def tabulate(source, carry):
        dy = lax.rem(source // 4 - y + 4, 4)
        dz = lax.rem(lax.rem(source, 4) - z + 4, 4)
        along = jnp.where(core == 0, dy, dz)
        across = jnp.where(core == 0, dz, dy)
        for s in range(2):
            near = send[along * SLOTS + here + s]
            table[source * 2 + s] = place_of(along, across, s, near)
        return carry

    lax.fori_loop(0, SLOTS // 2, tabulate, 0)

    def step(e, carry):
        for n in range(NODES):
            k = mode[n, e]
            f = flag[n, e]
            j = slot[n, e]
            w = root_of(levels[n, k])
            which = jnp.where(f >= 0, (n * OPS + lax.rem(k, 3)) * 2 + f, LISTS)
            count = counts[which]
            at = which * NEIGH + jnp.where(f >= 0, count, 0)
            counts[which] = count + 1
            codes[at] = table[j]
            codes[ROOM + at] = k
            values[at] = w
            values[ROOM + at] = w * coupling[0, k]
            values[2 * ROOM + at] = w * coupling[1, k]
        return carry

    lax.fori_loop(0, NEIGH, step, 0)


def prepare(slot, mode, flag, send, levels, damping, coupling, hamiltonian, couplers):
    return pl.pallas_call(
        prepare_kernel,
        out_shape=(
            jax.ShapeDtypeStruct((LISTS + 1,), jnp.int32),
            jax.ShapeDtypeStruct((2 * ROOM,), jnp.int32),
            jax.ShapeDtypeStruct((3 * ROOM,), jnp.float32),
            jax.ShapeDtypeStruct((NODES,), jnp.float32),
            jax.ShapeDtypeStruct(((OPS + 1) * WIDTH, WIDTH), jnp.bfloat16),
        ),
        in_specs=[smem()] * 7 + [pl.BlockSpec(memory_space=pltpu.VMEM)] * 2,
        out_specs=(smem(),) * 4 + (pl.BlockSpec(memory_space=pltpu.VMEM),),
        scratch_shapes=[SMEM((SLOTS,), jnp.int32)],
        cost_estimate=pl.CostEstimate(flops=2000000, bytes_accessed=20000, transcendentals=0),
        name="prepare",
    )(slot, mode, flag, send, levels, damping, coupling, hamiltonian, couplers)


def copy_through(reads, writes):
    for read in reads:
        read.start()
    for read, write in zip(reads, writes):
        read.wait()
        write.start()
    for write in writes:
        write.wait()


def across(hop):
    y, z, core = position()
    along_z = y * 4 + lax.rem(z + hop, 4)
    along_y = lax.rem(y + hop, 4) * 4 + z
    return jnp.where(core == 0, along_z, along_y) * 2


def pick_kernel(send, *refs):
    ins = refs[0:4]
    outs = refs[4:7]
    room, in_sem, out_sem = refs[7:]
    reads = []
    writes = []
    for i, hop in enumerate(HOPS):
        there = across(hop)
        for d in range(4):
            for s in range(2):
                at = d * 2 + s
                slot = i * 8 + at
                row = pl.multiple_of(send[d * SLOTS + there + s] * BLOCK, BLOCK)
                reads.append(
                    pltpu.make_async_copy(
                        ins[d].at[pl.ds(row, BLOCK)], room.at[slot], in_sem.at[slot]
                    )
                )
                writes.append(
                    pltpu.make_async_copy(room.at[slot], outs[i].at[at], out_sem.at[slot])
                )
    copy_through(reads, writes)


def pick(send, parts):
    shape = jax.ShapeDtypeStruct((8, BLOCK, WIDTH), jnp.bfloat16)
    return pl.pallas_call(
        pick_kernel,
        out_shape=(shape,) * 3,
        in_specs=[smem()] + [anywhere()] * 4,
        out_specs=(anywhere(),) * 3,
        scratch_shapes=[
            pltpu.VMEM((24, BLOCK, WIDTH), jnp.bfloat16),
            pltpu.SemaphoreType.DMA((24,)),
            pltpu.SemaphoreType.DMA((24,)),
        ],
        compiler_params=pltpu.CompilerParams(vmem_limit_bytes=VMEM_LIMIT),
        cost_estimate=pl.CostEstimate(flops=3000000, bytes_accessed=6 << 20, transcendentals=0),
        name="pick",
    )(send, *parts)


def row_of(chunk, half):
    return chunk * 2 * PIECE + half * PIECE


def rate_kernel(chunk, last, counts, codes, values, decay, operators_from, *refs):
    final = chunk == CHUNKS - 1
    own_from = refs[0:CHUNKS]
    refs = refs[CHUNKS:]
    if chunk > 0:
        before_from = refs[0]
        refs = refs[1:]
    sources = refs[0:7]
    refs = refs[7:]
    outs = CHUNKS if final and not last else 1
    out = refs[0:outs]
    grads, buffer, left, right, held, totals, sems, own, operators, *rest = refs[outs:]
    n = pl.program_id(0)

    copies = ([], [])
    for half in range(2):
        moves = []
        rows = pl.ds(half * PART, PART)
        for part in range(7):
            ref = sources[part]
            if part < 4:
                for m in range(NODES):
                    from_rows = pl.ds(m * BLOCK + half * PART, PART)
                    moves.append((ref.at[from_rows], buffer.at[part * 4 + m, rows]))
            else:
                places = pl.ds(16 + (part - 4) * 8, 8)
                moves.append((ref.at[:, rows], buffer.at[places, rows]))
        for i, (ref, to) in enumerate(moves):
            copies[half].append(pltpu.make_async_copy(ref, to, sems.at[half * 19 + i]))

    own_copies = [
        pltpu.make_async_copy(
            own_from[c].at[pl.ds(0, NODES * BLOCK)], own.at[c], sems.at[38 + c]
        )
        for c in range(CHUNKS)
    ]
    late_copies = [pltpu.make_async_copy(operators_from, operators, sems.at[38 + CHUNKS])]
    if chunk > 0:
        before = rest[0]
        late_copies.append(pltpu.make_async_copy(before_from, before, sems.at[39 + CHUNKS]))

    @pl.when(n == 0)
    def _():
        for copy in own_copies + copies[0] + copies[1] + late_copies:
            copy.start()
        totals[...] = jnp.zeros_like(totals)

    for half in range(2):
        mine = own.at[chunk, pl.ds(pl.multiple_of(n * BLOCK, BLOCK), BLOCK)]
        base = half * PART

        @pl.when(n == 0)
        def _(half=half):
            for copy in own_copies * (half == 0) + copies[half]:
                copy.wait()

        def block(i, carry, half=half, mine=mine, base=base):
            row = pl.multiple_of(i * ROWS, ROWS)
            here = pl.multiple_of(half * PIECE + i * ROWS, ROWS)
            own_real = mine[pl.ds(base + row, ROWS), :].astype(jnp.float32)
            own_imag = mine[pl.ds(base + PIECE + row, ROWS), :].astype(jnp.float32)
            held[0] = own_real
            held[1] = own_imag
            zero = jnp.zeros((ROWS, WIDTH), jnp.float32)
            left[0, pl.ds(here, ROWS), :] = (-own_imag).astype(jnp.bfloat16)
            left[1, pl.ds(here, ROWS), :] = own_real.astype(jnp.bfloat16)
            right[0, pl.ds(here, ROWS), 0:WIDTH] = (-own_imag).astype(jnp.bfloat16)
            right[1, pl.ds(here, ROWS), 0:WIDTH] = own_real.astype(jnp.bfloat16)
            for q in range(OPS):

                def entry(at):
                    place = codes[at]
                    mode = codes[ROOM + at]
                    return place, mode, values[at], values[ROOM + at], values[2 * ROOM + at]

                def load(now):
                    place, mode, w, u, v = now
                    real = buffer[place, pl.ds(half * PART + row, ROWS), :].astype(jnp.float32)
                    imag = buffer[place, pl.ds(half * PART + PIECE + row, ROWS), :].astype(jnp.float32)
                    product = held[0] * real + held[1] * imag
                    product = product[:, 0:128] + product[:, 128:256]
                    product = jnp.sum(product.reshape(ROWS // 8, 8, 128), axis=0)
                    totals[mode] = totals[mode] + w * product
                    return real, imag, u, v

                which = (n * OPS + q) * 2

                def raised(e, carry):
                    now, sum_real, sum_imag = carry
                    after = entry((which + 1) * NEIGH + e + 1)
                    real, imag, u, v = load(now)
                    return (
                        after,
                        sum_real + (u * real - v * imag),
                        sum_imag + (u * imag + v * real),
                    )

                def lowered(e, carry):
                    now, sum_real, sum_imag, turn_real, turn_imag = carry
                    after = entry(which * NEIGH + e + 1)
                    real, imag, u, v = load(now)
                    return (
                        after,
                        sum_real + u * real,
                        sum_imag + u * imag,
                        turn_real + v * real,
                        turn_imag + v * imag,
                    )

                start = entry((which + 1) * NEIGH)
                start_lowered = entry(which * NEIGH)
                _, sum_real, sum_imag = lax.fori_loop(
                    0, counts[which + 1], raised, (start, zero, zero)
                )
                _, sum_real, sum_imag, turn_real, turn_imag = lax.fori_loop(
                    0, counts[which], lowered, (start_lowered, sum_real, sum_imag, zero, zero)
                )
                at_row = pl.multiple_of((q + 1) * 2 * PIECE + here, ROWS)
                column = (q + 1) * WIDTH
                left[0, pl.ds(at_row, ROWS), :] = (sum_real - turn_imag).astype(jnp.bfloat16)
                left[1, pl.ds(at_row, ROWS), :] = (sum_imag + turn_real).astype(jnp.bfloat16)
                right[0, pl.ds(here, ROWS), column : column + WIDTH] = (
                    sum_real + turn_imag
                ).astype(jnp.bfloat16)
                right[1, pl.ds(here, ROWS), column : column + WIDTH] = (
                    sum_imag - turn_real
                ).astype(jnp.bfloat16)
            return carry

        lax.fori_loop(0, PIECE // ROWS, block, 0)

    @pl.when(n == 0)
    def _():
        for copy in late_copies:
            copy.wait()

    rate_decay = decay[n]
    columns = slice(chunk * 2 * PIECE, (chunk + 1) * 2 * PIECE)
    op_left = jnp.concatenate(
        [operators[q * WIDTH : (q + 1) * WIDTH, columns] for q in range(OPS + 1)], axis=1
    )
    for part in range(2):
        total = jnp.dot(op_left, left[part], preferred_element_type=jnp.float32)
        minus = jnp.dot(right[part], operators[...], preferred_element_type=jnp.float32)
        if chunk > 0:
            total += before[n, part]
        for c in range(CHUNKS):
            for half in range(2):
                rows = slice(row_of(c, half), row_of(c, half) + PIECE)
                value = total[rows]
                if c == chunk or (final and not last):
                    at = half * PART + part * PIECE
                    state = own[c, pl.ds(pl.multiple_of(n * BLOCK + at, PIECE), PIECE)].astype(
                        jnp.float32
                    )
                if c == chunk:
                    value -= minus[half * PIECE : (half + 1) * PIECE] + rate_decay * state
                if not final:
                    out[0][0, part, rows] = value
                elif last:
                    out[0][0, part, rows] = 0.25 * value
                else:
                    out[c][at : at + PIECE] = (state + 0.125 * value).astype(jnp.bfloat16)

    @pl.when(n == NODES - 1)
    def _():
        summed = jnp.sum(totals[...], axis=1)
        summed = jnp.sum(summed, axis=1, keepdims=True) * (1.0 / WIDTH)
        rows = lax.broadcasted_iota(jnp.int32, (MODES, 128), 0)
        lanes = lax.broadcasted_iota(jnp.int32, (MODES, 128), 1)
        grads[...] = jnp.sum(jnp.where(rows == lanes, summed, 0.0), axis=0, keepdims=True)


def rates(chunk, last, lists, decay, operators, own, before, sources):
    final = chunk == CHUNKS - 1
    counts, codes, values = lists
    whole = pl.BlockSpec((1, 2, WIDTH, WIDTH), lambda n: (n, 0, 0, 0))
    block = pl.BlockSpec((BLOCK, WIDTH), lambda n: (n, 0))
    if final and not last:
        outs = (jax.ShapeDtypeStruct((NODES * BLOCK, WIDTH), jnp.bfloat16),) * CHUNKS
        out_specs = (block,) * CHUNKS
    else:
        outs = (jax.ShapeDtypeStruct((NODES, 2, WIDTH, WIDTH), jnp.float32),)
        out_specs = (whole,)
    return pl.pallas_call(
        lambda *refs: rate_kernel(chunk, last, *refs),
        grid=(NODES,),
        out_shape=outs + (jax.ShapeDtypeStruct((1, 128), jnp.float32),),
        in_specs=[smem()] * 4
        + [anywhere()] * (8 + CHUNKS + (chunk > 0)),
        out_specs=out_specs + (pl.BlockSpec((1, 128), lambda n: (0, 0)),),
        scratch_shapes=[
            pltpu.VMEM((40, 2 * PART, WIDTH), jnp.bfloat16),
            pltpu.VMEM((2, (OPS + 1) * 2 * PIECE, WIDTH), jnp.bfloat16),
            pltpu.VMEM((2, 2 * PIECE, (OPS + 1) * WIDTH), jnp.bfloat16),
            pltpu.VMEM((2, ROWS, WIDTH), jnp.float32),
            pltpu.VMEM((MODES, 8, 128), jnp.float32),
            pltpu.SemaphoreType.DMA((40 + CHUNKS,)),
            pltpu.VMEM((CHUNKS, NODES * BLOCK, WIDTH), jnp.bfloat16),
            pltpu.VMEM(operators.shape, jnp.bfloat16),
        ]
        + [pltpu.VMEM((NODES, 2, WIDTH, WIDTH), jnp.float32)] * (chunk > 0),
        compiler_params=pltpu.CompilerParams(
            vmem_limit_bytes=VMEM_LIMIT, dimension_semantics=("arbitrary",)
        ),
        cost_estimate=pl.CostEstimate(
            flops=2 * 2 * 4 * 4 * WIDTH**3, bytes_accessed=8 << 20, transcendentals=0
        ),
        name="rates",
    )(counts, codes, values, decay, operators, *own, *before, *sources)


def over_all(value):
    copies = lax.optimization_barrier(jnp.broadcast_to(value[None], (DEVICES,) + value.shape))
    copies = lax.all_to_all(copies, TIER_MAT, 0, 0, tiled=True)
    return jnp.sum(lax.optimization_barrier(copies), axis=0)


def per_device(
    costate,
    hamiltonian,
    couplers,
    damping,
    coupling,
    levels,
    neighbour_slot,
    neighbour_mode,
    neighbour_flag,
    send_index,
):
    split = costate.reshape(NODES, 2, CHUNKS, 2, PIECE, WIDTH).transpose(2, 0, 3, 1, 4, 5)
    split = split.reshape(CHUNKS, NODES * BLOCK, WIDTH)
    label = jnp.pad(send_index.astype(jnp.bfloat16), ((0, 15), (0, WIDTH - SLOTS)))
    start = [jnp.concatenate([split[0], label])] + [split[c] for c in range(1, CHUNKS)]

    def section(own, last, tables):
        rings = []
        for c in range(CHUNKS):
            parts = [own[c]] * 4
            for offset in (1, 3, 2):
                parts[offset] = joint(own[c], 4 - offset, 0)
            rings.append(parts)
        if tables is None:
            held = lax.optimization_barrier(rings[0])
            send = jnp.concatenate([part[NODES * BLOCK, :SLOTS] for part in held]).astype(jnp.int32)
            *lists, decay, operators = prepare(
                neighbour_slot,
                neighbour_mode,
                neighbour_flag,
                send,
                levels,
                damping,
                coupling,
                hamiltonian,
                couplers,
            )
            tables = (send, lists, decay, operators)
        send, lists, decay, operators = tables
        far = []
        for c in range(CHUNKS):
            picked = pick(send, rings[c])
            come = {}
            for i, hop in enumerate(HOPS):
                come[4 - hop] = joint(picked[i], hop, 1)
            far.append(come)
        grads = 0.0
        before = ()
        for c in range(CHUNKS):
            sources = rings[c] + [far[c][d] for d in (1, 2, 3)]
            *before, grad = rates(c, last, lists, decay, operators, own, before, sources)
            grads = grads + grad
        return before, grads, tables

    middle, grad_first, tables = section(start, False, None)
    (increment,), grad_second, _ = section(middle, True, tables)
    gradient = over_all(grad_first + grad_second)
    return (increment, gradient[0, :MODES])


def solution(mesh):
    finer = Mesh(mesh.devices.reshape(4, 4, 4, 2), TIER_MAT)
    return jax.shard_map(
        per_device,
        mesh=finer,
        in_specs=(
            P(TIER_MAT, None, None, None),
            P(),
            P(),
            P(),
            P(),
            P(TIER_MAT, None),
            P(TIER_MAT, None),
            P(TIER_MAT, None),
            P(TIER_MAT, None),
            P(TIER_MAT, None),
        ),
        out_specs=(P(TIER_MAT, None, None, None), P()),
        check_vma=False,
    )
```
